8 devices in a mesh: dp: 2 (over y, z), tp: 4 (over x, core).
Axes of the slice: x: 2, y: 2, z: 1, core: 2. Of those that a mesh axis runs over, the one named last changes fastest.
Arguments:
- x: bfloat16 [128, 2560], P('dp'), parts along dimension 0
- k_cache: bfloat16 [128, 2048, 8, 128], P('dp', None, 'tp'), parts along dimension 0
- v_cache: bfloat16 [128, 2048, 8, 128], P('dp', None, 'tp'), parts along dimension 0
- gain_a: bfloat16 [2560], replicated
- wq: bfloat16 [2560, 4096], P(None, 'tp')
- wo: bfloat16 [4096, 2560], P('tp')
- gain_m: bfloat16 [2560], replicated
- w_gate: bfloat16 [2560, 9728], P(None, 'tp')
- w_up: bfloat16 [2560, 9728], P(None, 'tp')
- w_down: bfloat16 [9728, 2560], P('tp')
Outputs:
- output: bfloat16 [128, 2560], P('dp'), parts along dimension 0
There are 2 independent parts. The reference program is written for one: setup_inputs(seed, part) draws one part's arguments, and reference() takes and returns one part's arrays. A program takes and returns all parts, laid end to end along the dimension named above; an argument that names none is the same for every part.
All inputs are finite; a program needn't handle non-finite values.
Results may differ from the reference program's by a relative error of at most 0.017.
Values are sent between devices in bfloat16 or wider.
A program may use at most 2 GiB of HBM per device.

```python
import jax
import jax.numpy as jnp
from jax import lax

BATCH = 64
CACHE = 2048
D = 2560
HEADS = 32
KV_HEADS = 8
HEAD = 128
FF = 9728
THETA = 10000


def setup_inputs(seed: int = 0, part: int = 0) -> dict:
    kx, kc, kw, kn, kq, ko, km, kg, ku, kd = jax.random.split(jax.random.key(seed), 10)
    kx, kc, kw = (jax.random.fold_in(k, part) for k in (kx, kc, kw))

    def weights(key, rows, columns):
        return jax.random.normal(key, (rows, columns), jnp.float32) * rows**-0.5

    drawn = {
        "x": jax.random.normal(kx, (BATCH, D), jnp.float32),
        "k_cache": 2 * jax.random.normal(kc, (BATCH, CACHE, KV_HEADS, HEAD), jnp.float32),
        "v_cache": 4 * jax.random.normal(kw, (BATCH, CACHE, KV_HEADS, HEAD), jnp.float32),
        "gain_a": 1 + 0.1 * jax.random.normal(kn, (D,), jnp.float32),
        "wq": 2 * weights(kq, D, HEADS * HEAD),
        "wo": weights(ko, HEADS * HEAD, D),
        "gain_m": 1 + 0.1 * jax.random.normal(km, (D,), jnp.float32),
        "w_gate": weights(kg, D, FF),
        "w_up": weights(ku, D, FF),
        "w_down": 2 * weights(kd, FF, D),
    }
    return {k: v.astype(jnp.bfloat16) for k, v in drawn.items()}


def normed(x, gain):
    wide = x.astype(jnp.float32)
    scale = lax.rsqrt(jnp.mean(wide * wide, -1, keepdims=True) + 1e-6)
    return (wide * scale * gain.astype(jnp.float32)).astype(jnp.bfloat16)


def turned(t, place, theta):
    half = t.shape[-1] // 2
    angle = place.astype(jnp.float32)[:, None] * theta ** (-jnp.arange(half, dtype=jnp.float32) / half)
    cos, sin = jnp.cos(angle)[:, None], jnp.sin(angle)[:, None]
    a, b = t[..., :half].astype(jnp.float32), t[..., half:].astype(jnp.float32)
    return jnp.concatenate([a * cos - b * sin, b * cos + a * sin], -1).astype(jnp.bfloat16)


def matmul(a, w):
    return jnp.dot(a, w, preferred_element_type=jnp.float32).astype(jnp.bfloat16)


def einsum(form, a, b):
    return jnp.einsum(form, a.astype(jnp.float32), b.astype(jnp.float32))


def seen_by(a, wq, k_cache, v_cache, head, theta):
    batch, cache, kv_heads = k_cache.shape[:3]
    place = jnp.full((batch,), cache - 1)
    q = turned(matmul(a, wq).reshape(batch, -1, head), place, theta).reshape(batch, kv_heads, -1, head)
    scores = einsum("bgsd,bugd->bgsu", q, k_cache) * head**-0.5
    weights = jax.nn.softmax(scores, -1).astype(jnp.bfloat16)
    return einsum("bgsu,bugd->bgsd", weights, v_cache).astype(jnp.bfloat16).reshape(batch, -1)


def hidden_of(b, w_gate, w_up):
    gate = jnp.dot(b, w_gate, preferred_element_type=jnp.float32)
    up = jnp.dot(b, w_up, preferred_element_type=jnp.float32)
    return (jax.nn.silu(gate) * up).astype(jnp.bfloat16)


def reference(x, k_cache, v_cache, gain_a, wq, wo, gain_m, w_gate, w_up, w_down):
    seen = seen_by(normed(x, gain_a), wq, k_cache, v_cache, HEAD, THETA)
    h = (x.astype(jnp.float32) + jnp.dot(seen, wo, preferred_element_type=jnp.float32)).astype(jnp.bfloat16)
    hidden = hidden_of(normed(h, gain_m), w_gate, w_up)
    return (h.astype(jnp.float32) + jnp.dot(hidden, w_down, preferred_element_type=jnp.float32)).astype(jnp.bfloat16)
```

```python
import functools
import math

import jax
import jax.numpy as jnp
import numpy as np
from jax import lax
from jax.experimental import pallas as pl
from jax.experimental.pallas import tpu as pltpu
from jax.sharding import PartitionSpec as P

THETA = 10000
MESH = pl.DeviceIdType.MESH
F32, BF16 = jnp.float32, jnp.bfloat16

GROUP = 2
SLOTS = 8


def widths_of(total, width):
    return [(at, min(width, total - at)) for at in range(0, total, width)]


def rotary(head, place):
    half = head // 2
    angle = place * float(THETA) ** (-np.arange(half, dtype=np.float64) / half)
    cos, sin = np.cos(angle), np.sin(angle)
    rows = np.stack([np.concatenate([cos, cos]), np.concatenate([-sin, sin])])
    return np.broadcast_to(rows[:, None], (2, 8, head)).astype(np.float32)


def normed(x, gain):
    scale = lax.rsqrt(jnp.mean(x * x, -1, keepdims=True) + 1e-6)
    return (x * scale * gain).astype(BF16)


def layer(dims, x_hbm, k_hbm, v_hbm, ga_hbm, wq_hbm, wo_hbm, gm_hbm, wg_hbm, wu_hbm, wd_hbm, rot_hbm, y_ref, *scratch):
    batch, d, heads, kv, head, rows, ff = dims
    qcols = heads * head
    half = batch // 2
    ffw, dw, qw = widths_of(ff, 512), widths_of(d, 512), widths_of(qcols, 512)
    it = iter(scratch)

    def take(n):
        return [next(it) for _ in range(n)]

    (kbuf, vbuf, xbuf, gab, gmb, rot, abuf, qbuf, sa, sb, seen, hbuf, bbuf, hidden, part) = take(15)
    wob = take(len(dw))
    gb, ub = take(len(ffw)), take(len(ffw))
    db = take(len(dw))
    sends1, recvs1, sends2, recvs2, final = take(5)
    (small_sem, wq_sem, k_sem, v_sem, wo_sem, g_sem, u_sem, d_sem, ss1, rs1, ss2, rs2, ss3, rs3) = take(14)

    tp = lax.axis_index("tp")
    core = lax.rem(tp, 2)
    chip = lax.div(tp, 2)
    partner = chip * 2 + 1 - core
    across = (1 - chip) * 2 + core

    barrier = pltpu.get_barrier_semaphore()
    for other in (partner, across):
        pl.semaphore_signal(barrier, inc=1, device_id={"tp": other}, device_id_type=MESH)

    copy = pltpu.make_async_copy
    smalls = [copy(x_hbm, xbuf, small_sem.at[0]), copy(ga_hbm, gab, small_sem.at[1]), copy(gm_hbm, gmb, small_sem.at[2]), copy(rot_hbm, rot, small_sem.at[3])]
    for c in smalls:
        c.start()
    wqs = [copy(wq_hbm.at[:, pl.ds(at, w)], gb[i].at[:, pl.ds(0, w)], wq_sem.at[i]) for i, (at, w) in enumerate(qw)]
    for c in wqs:
        c.start()

    def k_copy(seq, slot):
        return copy(k_hbm.at[seq], kbuf.at[slot], k_sem.at[slot])

    def v_copy(seq, slot):
        return copy(v_hbm.at[seq], vbuf.at[slot], v_sem.at[slot])

    for s in range(SLOTS):
        k_copy(s, s).start()
        v_copy(s, s).start()

    wos = [copy(wo_hbm.at[:, pl.ds(at, w)], wob[i], wo_sem.at[i]) for i, (at, w) in enumerate(dw)]
    gs = [copy(wg_hbm.at[:, pl.ds(at, w)], gb[i], g_sem.at[i]) for i, (at, w) in enumerate(ffw)]
    us = [copy(wu_hbm.at[:, pl.ds(at, w)], ub[i], u_sem.at[i]) for i, (at, w) in enumerate(ffw)]
    ds = [copy(wd_hbm.at[:, pl.ds(at, w)], db[i], d_sem.at[i]) for i, (at, w) in enumerate(dw)]

    for c in smalls:
        c.wait()
    abuf[...] = normed(xbuf[...].astype(F32), gab[...].astype(F32))
    cos, sin = rot[0, 0:1, :], rot[1, 0:1, :]
    for i, (at, w) in enumerate(qw):
        wqs[i].wait()
        q = jnp.dot(abuf[...], gb[i][:, 0:w], preferred_element_type=F32)
        for n in range(w // head):
            t = q[:, n * head : (n + 1) * head].astype(BF16).astype(F32)
            t = t * cos + pltpu.roll(t, head // 2, 1) * sin
            qbuf[pl.ds(at // head + n, batch, stride=heads), :] = t.astype(BF16).astype(F32)

    groups = batch // GROUP
    ring = SLOTS // GROUP
    shape = (heads, rows)
    own = lax.rem(lax.broadcasted_iota(jnp.int32, shape, 1), kv) == lax.div(lax.broadcasted_iota(jnp.int32, shape, 0), heads // kv)
    factor = math.log2(math.e) * head**-0.5

    def slot_of(g, i):
        return lax.rem(g, ring) * GROUP + i

    def scores_of(g, out):
        for i in range(GROUP):
            q = qbuf[pl.ds(pl.multiple_of((g * GROUP + i) * heads, heads), heads), :].astype(BF16)
            s = lax.dot_general(q, kbuf[slot_of(g, i)], (((1,), (1,)), ((), ())), preferred_element_type=F32)
            out[i] = s

    def seen_of(g, scores):
        for i in range(GROUP):
            s = jnp.where(own, scores[i], -jnp.inf)
            p = jnp.exp2((s - jnp.max(s, -1, keepdims=True)) * factor)
            p = (p * (1.0 / jnp.sum(p, -1, keepdims=True))).astype(BF16)
            o = jnp.dot(p, vbuf[slot_of(g, i)], preferred_element_type=F32)
            seen[pl.ds(pl.multiple_of((g * GROUP + i) * heads, heads), heads), :] = o.astype(BF16).astype(F32)

    def wait_k(g):
        for i in range(GROUP):
            k_copy(g * GROUP + i, slot_of(g, i)).wait()

    def wait_v(g):
        for i in range(GROUP):
            v_copy(g * GROUP + i, slot_of(g, i)).wait()

    def start_k(g):
        for i in range(GROUP):
            k_copy(g * GROUP + i, slot_of(g, i)).start()

    def start_v(g):
        for i in range(GROUP):
            v_copy(g * GROUP + i, slot_of(g, i)).start()

    wait_k(0)
    scores_of(0, sa)

    def step(g, now, later, last=False):
        if not last:
            wait_k(g + 1)
        wait_v(g)
        if not last:
            scores_of(g + 1, later)
        seen_of(g, now)

        if not last:

            @pl.when(g == 0)
            def _():
                start_k(ring)

            @pl.when(g + 1 + ring < groups)
            def _():
                start_k(g + 1 + ring)

            @pl.when(g + ring < groups)
            def _():
                start_v(g + ring)

            @pl.when(g + ring == groups)
            def _():
                for c in wos:
                    c.start()
                for c in [c for pair in zip(gs, us) for c in pair] + ds:
                    c.start()

    def two(i, carry):
        step(2 * i, sa, sb)
        step(2 * i + 1, sb, sa)
        return carry

    lax.fori_loop(0, groups // 2 - 1, two, 0)
    step(groups - 2, sa, sb)
    step(groups - 1, sb, sa, last=True)

    pl.semaphore_wait(barrier, 2)

    mine = pl.ds(pl.multiple_of(core * half, half), half)
    theirs = pl.ds(pl.multiple_of((1 - core) * half, half), half)

    def remote(src, dst, send, recv, to):
        return pltpu.make_async_remote_copy(src_ref=src, dst_ref=dst, send_sem=send, recv_sem=recv, device_id={"tp": to}, device_id_type=MESH)

    def summed(which, term, base, out):
        n = len(dw)
        one = [remote(sends1.at[which, c], recvs1.at[which, c], ss1.at[which, c], rs1.at[which, c], partner) for c in range(n)]
        two_ = [remote(sends2.at[which, c], recvs2.at[which, c], ss2.at[which, c], rs2.at[which, c], across) for c in range(n)]
        three = [remote(out.at[c, mine, :], out.at[c, mine, :], ss3.at[which, c], rs3.at[which, c], partner) for c in range(n)]
        for c in range(n):
            part[c] = term(c)
            sends1[which, c] = part[c, theirs, :].astype(BF16)
            one[c].start()
        for c in range(n):
            one[c].wait_recv()
            sends2[which, c] = (part[c, mine, :] + recvs1[which, c].astype(F32)).astype(BF16)
            two_[c].start()
        for c in range(n):
            two_[c].wait_recv()
            total = sends2[which, c].astype(F32) + recvs2[which, c].astype(F32)
            out[c, mine, :] = (base(c) + total).astype(BF16)
            three[c].start()
        for c in range(n):
            three[c].wait()
            one[c].wait_send()
            two_[c].wait_send()

    for n in range(heads):
        hidden[:, n * head : (n + 1) * head] = seen[pl.ds(n, batch, stride=heads), :].astype(BF16)

    def wo_term(c):
        wos[c].wait()
        return jnp.dot(hidden[:, 0:qcols], wob[c][...], preferred_element_type=F32)

    summed(0, wo_term, lambda c: xbuf[mine, pl.ds(dw[c][0], dw[c][1])].astype(F32), hbuf)

    squares = jnp.zeros((batch, 1), F32)
    for c in range(len(dw)):
        h = hbuf[c].astype(F32)
        squares = squares + jnp.sum(h * h, -1, keepdims=True)
    scale = lax.rsqrt(squares * (1.0 / d) + 1e-6)
    for c, (at, w) in enumerate(dw):
        bbuf[:, at : at + w] = (hbuf[c].astype(F32) * scale * gmb[:, at : at + w].astype(F32)).astype(BF16)

    for c, (at, w) in enumerate(ffw):
        gs[c].wait()
        us[c].wait()
        gate = jnp.dot(bbuf[...], gb[c][...], preferred_element_type=F32)
        up = jnp.dot(bbuf[...], ub[c][...], preferred_element_type=F32)
        hidden[:, at : at + w] = (gate * (1.0 / (1.0 + jnp.exp(-gate))) * up).astype(BF16)

    def down_term(c):
        ds[c].wait()
        return jnp.dot(hidden[...], db[c][...], preferred_element_type=F32)

    summed(1, down_term, lambda c: hbuf[c, mine, :].astype(F32), final)
    for c, (at, w) in enumerate(dw):
        y_ref[:, at : at + w] = final[c]


def solution(mesh):
    def step(x, k_cache, v_cache, gain_a, wq, wo, gain_m, w_gate, w_up, w_down):
        batch, cache, kv, head = k_cache.shape
        d, qcols = wq.shape
        heads, ff, rows = qcols // head, w_gate.shape[1], cache * kv
        dims = (batch, d, heads, kv, head, rows, ff)
        half = batch // 2
        ffw, dw = widths_of(ff, 512), widths_of(d, 512)
        n, w = len(dw), dw[0][1]
        dma = pltpu.SemaphoreType.DMA
        scratch = [
            pltpu.VMEM((SLOTS, rows, head), BF16),
            pltpu.VMEM((SLOTS, rows, head), BF16),
            pltpu.VMEM((batch, d), BF16),
            pltpu.VMEM((1, d), BF16),
            pltpu.VMEM((1, d), BF16),
            pltpu.VMEM((2, 8, head), F32),
            pltpu.VMEM((batch, d), BF16),
            pltpu.VMEM((batch * heads, head), F32),
            pltpu.VMEM((GROUP, heads, rows), F32),
            pltpu.VMEM((GROUP, heads, rows), F32),
            pltpu.VMEM((batch * heads, head), F32),
            pltpu.VMEM((n, batch, w), BF16),
            pltpu.VMEM((batch, d), BF16),
            pltpu.VMEM((batch, ff), BF16),
            pltpu.VMEM((n, batch, w), F32),
            *[pltpu.VMEM((qcols, w), BF16) for _, w in dw],
            *[pltpu.VMEM((d, w), BF16) for _, w in ffw],
            *[pltpu.VMEM((d, w), BF16) for _, w in ffw],
            *[pltpu.VMEM((ff, w), BF16) for _, w in dw],
            *[pltpu.VMEM((2, n, half, w), BF16) for _ in range(4)],
            pltpu.VMEM((n, batch, w), BF16),
            dma((4,)),
            dma((2,)),
            dma((SLOTS,)),
            dma((SLOTS,)),
            dma((n,)),
            dma((len(ffw),)),
            dma((len(ffw),)),
            dma((n,)),
            *[dma((2, n)) for _ in range(6)],
        ]
        hbm = pl.BlockSpec(memory_space=pltpu.HBM)
        return pl.pallas_call(
            functools.partial(layer, dims),
            out_shape=jax.ShapeDtypeStruct((batch, d), BF16),
            in_specs=[hbm] * 11,
            out_specs=pl.BlockSpec(memory_space=pltpu.VMEM),
            scratch_shapes=scratch,
            compiler_params=pltpu.CompilerParams(collective_id=0, has_side_effects=True, vmem_limit_bytes=67043328),
            name="decoder_layer",
        )(
            x,
            k_cache.reshape(batch, rows, head),
            v_cache.reshape(batch, rows, head),
            gain_a.reshape(1, d),
            wq,
            wo,
            gain_m.reshape(1, d),
            w_gate,
            w_up,
            w_down,
            rotary(head, cache - 1),
        )

    states, cache, columns, rows_of = P("dp", None), P("dp", None, "tp", None), P(None, "tp"), P("tp", None)
    return jax.shard_map(
        step,
        mesh=mesh,
        in_specs=(states, cache, cache, P(None), columns, rows_of, P(None), columns, columns, rows_of),
        out_specs=states,
        check_vma=False,
    )
```

```python
import functools
import math

import jax
import jax.numpy as jnp
import numpy as np
from jax import lax
from jax.experimental import pallas as pl
from jax.experimental.pallas import tpu as pltpu
from jax.sharding import PartitionSpec as P

THETA = 10000
MESH = pl.DeviceIdType.MESH
F32, BF16 = jnp.float32, jnp.bfloat16

GROUP = 2
SLOTS = 8


def widths_of(total, width):
    return [(at, min(width, total - at)) for at in range(0, total, width)]


def rotary(head, place):
    half = head // 2
    angle = place * float(THETA) ** (-np.arange(half, dtype=np.float64) / half)
    cos, sin = np.cos(angle), np.sin(angle)
    rows = np.stack([np.concatenate([cos, cos]), np.concatenate([-sin, sin])])
    return np.broadcast_to(rows[:, None], (2, 8, head)).astype(np.float32)


def row_of(gain):
    wide = gain[...].astype(F32)
    return jnp.concatenate([wide[n : n + 1] for n in range(wide.shape[0])], -1)


def normed(x, gain):
    scale = lax.rsqrt(jnp.mean(x * x, -1, keepdims=True) + 1e-6)
    return (x * scale * gain).astype(BF16)


def layer(dims, x_hbm, k_hbm, v_hbm, ga_hbm, wq_hbm, wo_hbm, gm_hbm, wg_hbm, wu_hbm, wd_hbm, rot_hbm, y_ref, *scratch):
    batch, d, heads, kv, head, rows, ff = dims
    qcols = heads * head
    half = batch // 2
    ffw, dw, qw = widths_of(ff, 512), widths_of(d, 512), widths_of(qcols, 512)
    it = iter(scratch)

    def take(n):
        return [next(it) for _ in range(n)]

    (kbuf, vbuf, xbuf, gab, gmb, rot, abuf, qbuf, sa, sb, seen, hbuf, bbuf, hidden, part) = take(15)
    wob = take(len(dw))
    gb, ub = take(len(ffw)), take(len(ffw))
    db = take(len(dw))
    sends1, recvs1, sends2, recvs2, final = take(5)
    (small_sem, wq_sem, k_sem, v_sem, wo_sem, g_sem, u_sem, d_sem, ss1, rs1, ss2, rs2, ss3, rs3) = take(14)

    tp = lax.axis_index("tp")
    core = lax.rem(tp, 2)
    chip = lax.div(tp, 2)
    partner = chip * 2 + 1 - core
    across = (1 - chip) * 2 + core

    barrier = pltpu.get_barrier_semaphore()
    for other in (partner, across):
        pl.semaphore_signal(barrier, inc=1, device_id={"tp": other}, device_id_type=MESH)

    copy = pltpu.make_async_copy
    smalls = [copy(x_hbm, xbuf, small_sem.at[0]), copy(ga_hbm, gab, small_sem.at[1]), copy(gm_hbm, gmb, small_sem.at[2]), copy(rot_hbm, rot, small_sem.at[3])]
    for c in smalls:
        c.start()
    wqs = [copy(wq_hbm.at[:, pl.ds(at, w)], gb[i].at[:, pl.ds(0, w)], wq_sem.at[i]) for i, (at, w) in enumerate(qw)]
    for c in wqs:
        c.start()

    def k_copy(seq, slot):
        return copy(k_hbm.at[seq], kbuf.at[slot], k_sem.at[slot])

    def v_copy(seq, slot):
        return copy(v_hbm.at[seq], vbuf.at[slot], v_sem.at[slot])

    for s in range(SLOTS):
        k_copy(s, s).start()
        v_copy(s, s).start()

    wos = [copy(wo_hbm.at[:, pl.ds(at, w)], wob[i], wo_sem.at[i]) for i, (at, w) in enumerate(dw)]
    gs = [copy(wg_hbm.at[:, pl.ds(at, w)], gb[i], g_sem.at[i]) for i, (at, w) in enumerate(ffw)]
    us = [copy(wu_hbm.at[:, pl.ds(at, w)], ub[i], u_sem.at[i]) for i, (at, w) in enumerate(ffw)]
    ds = [copy(wd_hbm.at[:, pl.ds(at, w)], db[i], d_sem.at[i]) for i, (at, w) in enumerate(dw)]

    for c in smalls:
        c.wait()
    abuf[...] = normed(xbuf[...].astype(F32), row_of(gab))
    cos, sin = rot[0, 0:1, :], rot[1, 0:1, :]
    for i, (at, w) in enumerate(qw):
        wqs[i].wait()
        q = jnp.dot(abuf[...], gb[i][:, 0:w], preferred_element_type=F32)
        for n in range(w // head):
            t = q[:, n * head : (n + 1) * head].astype(BF16).astype(F32)
            t = t * cos + pltpu.roll(t, head // 2, 1) * sin
            qbuf[pl.ds(at // head + n, batch, stride=heads), :] = t.astype(BF16).astype(F32)

    groups = batch // GROUP
    ring = SLOTS // GROUP
    shape = (heads, rows)
    own = lax.rem(lax.broadcasted_iota(jnp.int32, shape, 1), kv) == lax.div(lax.broadcasted_iota(jnp.int32, shape, 0), heads // kv)
    factor = math.log2(math.e) * head**-0.5

    def slot_of(g, i):
        return lax.rem(g, ring) * GROUP + i

    def scores_of(g, out):
        for i in range(GROUP):
            q = qbuf[pl.ds(pl.multiple_of((g * GROUP + i) * heads, heads), heads), :].astype(BF16)
            s = lax.dot_general(q, kbuf[slot_of(g, i)], (((1,), (1,)), ((), ())), preferred_element_type=F32)
            out[i] = s

    def seen_of(g, scores):
        for i in range(GROUP):
            s = jnp.where(own, scores[i], -jnp.inf)
            p = jnp.exp2((s - jnp.max(s, -1, keepdims=True)) * factor)
            p = (p * (1.0 / jnp.sum(p, -1, keepdims=True))).astype(BF16)
            o = jnp.dot(p, vbuf[slot_of(g, i)], preferred_element_type=F32)
            seen[pl.ds(pl.multiple_of((g * GROUP + i) * heads, heads), heads), :] = o.astype(BF16).astype(F32)

    def wait_k(g):
        for i in range(GROUP):
            k_copy(g * GROUP + i, slot_of(g, i)).wait()

    def wait_v(g):
        for i in range(GROUP):
            v_copy(g * GROUP + i, slot_of(g, i)).wait()

    def start_k(g):
        for i in range(GROUP):
            k_copy(g * GROUP + i, slot_of(g, i)).start()

    def start_v(g):
        for i in range(GROUP):
            v_copy(g * GROUP + i, slot_of(g, i)).start()

    wait_k(0)
    scores_of(0, sa)

    def step(g, now, later, last=False):
        if not last:
            wait_k(g + 1)
        wait_v(g)
        if not last:
            scores_of(g + 1, later)
        seen_of(g, now)

        if not last:

            @pl.when(g == 0)
            def _():
                start_k(ring)

            @pl.when(g + 1 + ring < groups)
            def _():
                start_k(g + 1 + ring)

            @pl.when(g + ring < groups)
            def _():
                start_v(g + ring)

            @pl.when(g + ring == groups)
            def _():
                for c in wos:
                    c.start()
                for c in [c for pair in zip(gs, us) for c in pair] + ds:
                    c.start(priority=1)

    def two(i, carry):
        step(2 * i, sa, sb)
        step(2 * i + 1, sb, sa)
        return carry

    lax.fori_loop(0, groups // 2 - 1, two, 0)
    step(groups - 2, sa, sb)
    step(groups - 1, sb, sa, last=True)

    pl.semaphore_wait(barrier, 2)

    mine = pl.ds(pl.multiple_of(core * half, half), half)
    theirs = pl.ds(pl.multiple_of((1 - core) * half, half), half)

    def remote(src, dst, send, recv, to):
        return pltpu.make_async_remote_copy(src_ref=src, dst_ref=dst, send_sem=send, recv_sem=recv, device_id={"tp": to}, device_id_type=MESH)

    def summed(which, term, base, out):
        n = len(dw)
        one = [remote(sends1.at[which, c], recvs1.at[which, c], ss1.at[which, c], rs1.at[which, c], partner) for c in range(n)]
        two_ = [remote(sends2.at[which, c], recvs2.at[which, c], ss2.at[which, c], rs2.at[which, c], across) for c in range(n)]
        three = [remote(out.at[c, mine, :], out.at[c, mine, :], ss3.at[which, c], rs3.at[which, c], partner) for c in range(n)]
        for c in range(n):
            part[c] = term(c)
            sends1[which, c] = part[c, theirs, :].astype(BF16)
            one[c].start()
        for c in range(n):
            one[c].wait_recv()
            sends2[which, c] = (part[c, mine, :] + recvs1[which, c].astype(F32)).astype(BF16)
            two_[c].start()
        for c in range(n):
            two_[c].wait_recv()
            total = sends2[which, c].astype(F32) + recvs2[which, c].astype(F32)
            out[c, mine, :] = (base(c) + total).astype(BF16)
            three[c].start()
        for c in range(n):
            three[c].wait()
            one[c].wait_send()
            two_[c].wait_send()

    for n in range(heads):
        hidden[:, n * head : (n + 1) * head] = seen[pl.ds(n, batch, stride=heads), :].astype(BF16)

    def wo_term(c):
        wos[c].wait()
        return jnp.dot(hidden[:, 0:qcols], wob[c][...], preferred_element_type=F32)

    summed(0, wo_term, lambda c: xbuf[mine, pl.ds(dw[c][0], dw[c][1])].astype(F32), hbuf)

    squares = jnp.zeros((batch, 1), F32)
    for c in range(len(dw)):
        h = hbuf[c].astype(F32)
        squares = squares + jnp.sum(h * h, -1, keepdims=True)
    scale = lax.rsqrt(squares * (1.0 / d) + 1e-6)
    gain = row_of(gmb)
    for c, (at, w) in enumerate(dw):
        bbuf[:, at : at + w] = (hbuf[c].astype(F32) * scale * gain[:, at : at + w]).astype(BF16)

    for c, (at, w) in enumerate(ffw):
        gs[c].wait()
        us[c].wait()
        gate = jnp.dot(bbuf[...], gb[c][...], preferred_element_type=F32)
        up = jnp.dot(bbuf[...], ub[c][...], preferred_element_type=F32)
        hidden[:, at : at + w] = (gate * (1.0 / (1.0 + jnp.exp(-gate))) * up).astype(BF16)

    def down_term(c):
        ds[c].wait()
        return jnp.dot(hidden[...], db[c][...], preferred_element_type=F32)

    summed(1, down_term, lambda c: hbuf[c, mine, :].astype(F32), final)
    for c, (at, w) in enumerate(dw):
        y_ref[:, at : at + w] = final[c]


def solution(mesh):
    def step(x, k_cache, v_cache, gain_a, wq, wo, gain_m, w_gate, w_up, w_down):
        batch, cache, kv, head = k_cache.shape
        d, qcols = wq.shape
        heads, ff, rows = qcols // head, w_gate.shape[1], cache * kv
        dims = (batch, d, heads, kv, head, rows, ff)
        half = batch // 2
        ffw, dw = widths_of(ff, 512), widths_of(d, 512)
        n, w = len(dw), dw[0][1]
        dma = pltpu.SemaphoreType.DMA
        scratch = [
            pltpu.VMEM((SLOTS, rows, head), BF16),
            pltpu.VMEM((SLOTS, rows, head), BF16),
            pltpu.VMEM((batch, d), BF16),
            pltpu.VMEM((d // 128, 128), BF16),
            pltpu.VMEM((d // 128, 128), BF16),
            pltpu.VMEM((2, 8, head), F32),
            pltpu.VMEM((batch, d), BF16),
            pltpu.VMEM((batch * heads, head), F32),
            pltpu.VMEM((GROUP, heads, rows), F32),
            pltpu.VMEM((GROUP, heads, rows), F32),
            pltpu.VMEM((batch * heads, head), F32),
            pltpu.VMEM((n, batch, w), BF16),
            pltpu.VMEM((batch, d), BF16),
            pltpu.VMEM((batch, ff), BF16),
            pltpu.VMEM((n, batch, w), F32),
            *[pltpu.VMEM((qcols, w), BF16) for _, w in dw],
            *[pltpu.VMEM((d, w), BF16) for _, w in ffw],
            *[pltpu.VMEM((d, w), BF16) for _, w in ffw],
            *[pltpu.VMEM((ff, w), BF16) for _, w in dw],
            *[pltpu.VMEM((2, n, half, w), BF16) for _ in range(4)],
            pltpu.VMEM((n, batch, w), BF16),
            dma((4,)),
            dma((2,)),
            dma((SLOTS,)),
            dma((SLOTS,)),
            dma((n,)),
            dma((len(ffw),)),
            dma((len(ffw),)),
            dma((n,)),
            *[dma((2, n)) for _ in range(6)],
        ]
        hbm = pl.BlockSpec(memory_space=pltpu.HBM)
        return pl.pallas_call(
            functools.partial(layer, dims),
            out_shape=pltpu.VMEM((batch, d), BF16),
            in_specs=[hbm] * 11,
            out_specs=pl.BlockSpec(memory_space=pltpu.VMEM),
            scratch_shapes=scratch,
            compiler_params=pltpu.CompilerParams(collective_id=0, has_side_effects=True, vmem_limit_bytes=66000000),
            name="decoder_layer",
        )(
            x,
            k_cache.reshape(batch, rows, head),
            v_cache.reshape(batch, rows, head),
            gain_a.reshape(d // 128, 128),
            wq,
            wo,
            gain_m.reshape(d // 128, 128),
            w_gate,
            w_up,
            w_down,
            rotary(head, cache - 1),
        )

    states, cache, columns, rows_of = P("dp", None), P("dp", None, "tp", None), P(None, "tp"), P("tp", None)
    return jax.shard_map(
        step,
        mesh=mesh,
        in_specs=(states, cache, cache, P(None), columns, rows_of, P(None), columns, columns, rows_of),
        out_specs=states,
        check_vma=False,
    )
```

```python
import functools
import math

import jax
import jax.numpy as jnp
import numpy as np
from jax import lax
from jax.experimental import pallas as pl
from jax.experimental.pallas import tpu as pltpu
from jax.sharding import PartitionSpec as P

THETA = 10000
MESH = pl.DeviceIdType.MESH
F32, BF16 = jnp.float32, jnp.bfloat16

GROUP = 2
SLOTS = 8
LAG = 2
BLOCK = 8


def widths_of(total, width):
    return [(at, min(width, total - at)) for at in range(0, total, width)]


def rotary(head, place):
    half = head // 2
    angle = place * float(THETA) ** (-np.arange(half, dtype=np.float64) / half)
    cos, sin = np.cos(angle), np.sin(angle)
    rows = np.stack([np.concatenate([cos, cos]), np.concatenate([-sin, sin])])
    return np.broadcast_to(rows[:, None], (2, 8, head)).astype(np.float32)


def row_of(gain):
    wide = gain[...].astype(F32)
    return jnp.concatenate([wide[n : n + 1] for n in range(wide.shape[0])], -1)


def normed(x, gain):
    scale = lax.rsqrt(jnp.mean(x * x, -1, keepdims=True) + 1e-6)
    return (x * scale * gain).astype(BF16)


def layer(dims, x_hbm, k_hbm, v_hbm, ga_hbm, wq_hbm, wo_hbm, gm_hbm, wg_hbm, wu_hbm, wd_hbm, rot_hbm, y_ref, *scratch):
    batch, d, heads, kv, head, rows, ff = dims
    qcols = heads * head
    half = batch // 2
    ffw, dw, qw, ow = widths_of(ff, 512), widths_of(d, 512), widths_of(qcols, 512), widths_of(d, d // 2)
    it = iter(scratch)

    def take(n):
        return [next(it) for _ in range(n)]

    (kbuf, vbuf, xbuf, gab, gmb, rot, bbuf, qbuf, sa, sb, seen, states, wide, hidden) = take(14)
    wob = take(len(ow))
    gb, ub = take(len(ffw)), take(len(ffw))
    db = take(len(dw))
    terms, others, sends1, recvs1, sends2, recvs2 = take(6)
    (small_sem, wq_sem, k_sem, v_sem, wo_sem, g_sem, u_sem, d_sem, ts, tr, ss1, rs1, ss2, rs2, ss3, rs3) = take(16)

    tp = lax.axis_index("tp")
    core = lax.rem(tp, 2)
    chip = lax.div(tp, 2)
    partner = chip * 2 + 1 - core
    across = (1 - chip) * 2 + core
    diagonal = (1 - chip) * 2 + 1 - core
    peers = (partner, across, diagonal)

    barrier = pltpu.get_barrier_semaphore()
    for other in peers:
        pl.semaphore_signal(barrier, inc=1, device_id={"tp": other}, device_id_type=MESH)

    copy = pltpu.make_async_copy
    smalls = [copy(x_hbm, xbuf, small_sem.at[0]), copy(ga_hbm, gab, small_sem.at[1]), copy(gm_hbm, gmb, small_sem.at[2]), copy(rot_hbm, rot, small_sem.at[3])]
    for c in smalls:
        c.start()
    wqs = [copy(wq_hbm.at[:, pl.ds(at, w)], gb[i].at[:, pl.ds(0, w)], wq_sem.at[i]) for i, (at, w) in enumerate(qw)]
    for c in wqs:
        c.start()

    def k_copy(seq, slot):
        return copy(k_hbm.at[seq], kbuf.at[slot], k_sem.at[slot])

    def v_copy(seq, slot):
        return copy(v_hbm.at[seq], vbuf.at[slot], v_sem.at[slot])

    for s in range(SLOTS):
        k_copy(s, s).start()
        v_copy(s, s).start()

    wos = [copy(wo_hbm.at[:, pl.ds(at, w)], wob[i], wo_sem.at[i]) for i, (at, w) in enumerate(ow)]
    gs = [copy(wg_hbm.at[:, pl.ds(at, w)], gb[i], g_sem.at[i]) for i, (at, w) in enumerate(ffw)]
    us = [copy(wu_hbm.at[:, pl.ds(at, w)], ub[i], u_sem.at[i]) for i, (at, w) in enumerate(ffw)]
    ds = [copy(wd_hbm.at[:, pl.ds(at, w)], db[i], d_sem.at[i]) for i, (at, w) in enumerate(dw)]
    for c in wos:
        c.start()

    for c in smalls:
        c.wait()
    states[...] = xbuf[...].astype(F32)
    bbuf[...] = normed(states[...], row_of(gab)).astype(BF16)
    cos, sin = rot[0, 0:1, :], rot[1, 0:1, :]
    for i, (at, w) in enumerate(qw):
        wqs[i].wait()
        q = jnp.dot(bbuf[...], gb[i][:, 0:w], preferred_element_type=F32)
        for n in range(w // head):
            t = q[:, n * head : (n + 1) * head].astype(BF16).astype(F32)
            t = t * cos + pltpu.roll(t, head // 2, 1) * sin
            qbuf[pl.ds(at // head + n, batch, stride=heads), :] = t.astype(BF16).astype(F32)

    groups = batch // GROUP
    ring = SLOTS // GROUP
    shape = (heads, rows)
    own = lax.rem(lax.broadcasted_iota(jnp.int32, shape, 1), kv) == lax.div(lax.broadcasted_iota(jnp.int32, shape, 0), heads // kv)
    factor = math.log2(math.e) * head**-0.5

    def slot_of(g, i):
        return lax.rem(g, ring) * GROUP + i

    def rows_of(g, i):
        return pl.ds(pl.multiple_of((g * GROUP + i) * heads, heads), heads)

    def scores_of(g, out):
        for i in range(GROUP):
            q = qbuf[rows_of(g, i), :].astype(BF16)
            out[i] = lax.dot_general(q, kbuf[slot_of(g, i)], (((1,), (1,)), ((), ())), preferred_element_type=F32)

    def weights_of(scores, i):
        s = jnp.where(own, scores[i], -jnp.inf)
        p = jnp.exp2((s - jnp.max(s, -1, keepdims=True)) * factor)
        return (p * (1.0 / jnp.sum(p, -1, keepdims=True))).astype(BF16)

    def seen_of(g, i, p):
        o = jnp.dot(p, vbuf[slot_of(g, i)], preferred_element_type=F32)
        seen[rows_of(g, i), :] = o.astype(BF16).astype(F32)

    def wait_k(g):
        for i in range(GROUP):
            k_copy(g * GROUP + i, slot_of(g, i)).wait()

    def wait_v(g, i):
        v_copy(g * GROUP + i, slot_of(g, i)).wait()

    def start_k(g):
        for i in range(GROUP):
            k_copy(g * GROUP + i, slot_of(g, i)).start()

    def start_v(g):
        for i in range(GROUP):
            v_copy(g * GROUP + i, slot_of(g, i)).start()

    def step(g, now, later):
        wait_k(g + 1)
        for i in range(GROUP):
            wait_v(g, i)
        scores_of(g + 1, later)
        for i in range(GROUP):
            seen_of(g, i, weights_of(now, i))

        @pl.when(g + 1 + ring < groups)
        def _():
            start_k(g + 1 + ring)

        @pl.when(g + ring < groups)
        def _():
            start_v(g + ring)

        @pl.when(g + ring == groups)
        def _():
            for c in [c for pair in zip(gs, us) for c in pair]:
                c.start(priority=1)

    def tail(g, now, later):
        wait_k(g + 1)
        scores_of(g + 1, later)
        ps = [weights_of(scores, i) for scores in (now, later) for i in range(GROUP)]
        for m in range(2):
            for i in range(GROUP):
                wait_v(g + m, i)
                seen_of(g + m, i, ps[m * GROUP + i])

    def remote(src, dst, send, recv, to):
        return pltpu.make_async_remote_copy(src_ref=src, dst_ref=dst, send_sem=send, recv_sem=recv, device_id={"tp": to}, device_id_type=MESH)

    def exchanges(b, n, c):
        at = pl.ds(b, n)
        return [remote(terms.at[c, at], others.at[p, c, at], ts.at[p, c, b], tr.at[p, c, b], to) for p, to in enumerate(peers)]

    def send_terms(b, n):
        rows = n * BLOCK
        block = [seen[pl.ds(b * (BLOCK * heads) + m, rows, stride=heads), :] for m in range(heads)]
        block = jnp.concatenate(block, -1).astype(BF16)
        for c, (at, w) in enumerate(ow):
            term = jnp.dot(block, wob[c][...], preferred_element_type=F32)
            terms[c, pl.ds(b, n)] = term.reshape(n, BLOCK, w).astype(BF16)
            for e in exchanges(b, n, c):
                e.start()

    def add_terms(b, n):
        rows = n * BLOCK
        at_rows = pl.ds(b * BLOCK, rows)
        squares = jnp.zeros((rows, 1), F32)
        for c, (at, w) in enumerate(ow):
            for e in exchanges(b, n, c):
                e.wait()
            t = [terms[c, pl.ds(b, n)]] + [others[p, c, pl.ds(b, n)] for p in range(3)]
            t = [v.astype(F32).reshape(rows, w) for v in t]
            h = states[at_rows, at : at + w] + ((t[0] + t[1]) + (t[2] + t[3]))
            h = h.astype(BF16).astype(F32)
            states[at_rows, at : at + w] = h
            squares = squares + jnp.sum(h * h, -1, keepdims=True)
        scale = lax.rsqrt(squares * (1.0 / d) + 1e-6)
        wide[at_rows, :] = states[at_rows, :] * scale * row_of(gmb)

    wait_k(0)
    scores_of(0, sa)
    start_k(ring)
    for c in wos:
        c.wait()
    pl.semaphore_wait(barrier, 3)
    trips, blocks = groups // 2, batch // BLOCK
    ahead = 2 * BLOCK // (2 * GROUP)
    early = blocks - 2

    def two(i, carry):
        step(2 * i, sa, sb)
        step(2 * i + 1, sb, sa)

        @pl.when(jnp.logical_and(lax.rem(i, ahead) == ahead - 1, i < trips - ahead))
        def _():
            send_terms(lax.div(i, ahead) * 2, 2)

        @pl.when(i == trips - 1 - ahead // 2)
        def _():
            send_terms(early, 1)

        return carry

    lax.fori_loop(0, trips - 1, two, 0)
    tail(groups - 2, sa, sb)
    send_terms(blocks - 1, 1)
    for c in ds:
        c.start(priority=1)
    for b in range(0, early, 2):
        add_terms(b, 2)
    add_terms(early, 1)
    add_terms(early + 1, 1)
    bbuf[...] = wide[...].astype(BF16)

    for c, (at, w) in enumerate(ffw):
        gs[c].wait()
        us[c].wait()
        gate = jnp.dot(bbuf[...], gb[c][...], preferred_element_type=F32)
        up = jnp.dot(bbuf[...], ub[c][...], preferred_element_type=F32)
        hidden[:, at : at + w] = (gate * (1.0 / (1.0 + jnp.exp(-gate))) * up).astype(BF16)

    which = lax.rem(core + chip, 2)
    mine = pl.ds(pl.multiple_of(which * half, half), half)
    theirs = pl.ds(pl.multiple_of((1 - which) * half, half), half)
    n = len(dw)
    one = [remote(sends1.at[c], recvs1.at[c], ss1.at[c], rs1.at[c], partner) for c in range(n)]
    two = [remote(sends2.at[c], recvs2.at[c], ss2.at[c], rs2.at[c], diagonal) for c in range(n)]
    spots = [y_ref.at[mine, pl.ds(at, w)] for at, w in dw]
    three = [remote(spots[c], spots[c], ss3.at[c], rs3.at[c], partner) for c in range(n)]

    def send_half(c):
        at, w = dw[c]
        wide[:, at : at + w] = jnp.dot(hidden[...], db[c][...], preferred_element_type=F32)
        sends1[c] = wide[theirs, at : at + w].astype(BF16)
        one[c].start()

    def send_chip(c):
        at, w = dw[c]
        one[c].wait_recv()
        sends2[c] = (wide[mine, at : at + w] + recvs1[c].astype(F32)).astype(BF16)
        two[c].start()

    def finish(c):
        at, w = dw[c]
        two[c].wait_recv()
        y_ref[mine, at : at + w] = (states[mine, at : at + w] + (sends2[c].astype(F32) + recvs2[c].astype(F32))).astype(BF16)
        three[c].start()

    for c in range(n + LAG):
        if c < n:
            ds[c].wait()
            send_half(c)
        if c >= LAG:
            send_chip(c - LAG)
    for c in range(n):
        finish(c)
    for c in range(n):
        three[c].wait()
        one[c].wait_send()
        two[c].wait_send()


def solution(mesh):
    def step(x, k_cache, v_cache, gain_a, wq, wo, gain_m, w_gate, w_up, w_down):
        batch, cache, kv, head = k_cache.shape
        d, qcols = wq.shape
        heads, ff, rows = qcols // head, w_gate.shape[1], cache * kv
        dims = (batch, d, heads, kv, head, rows, ff)
        half = batch // 2
        ffw, dw, ow = widths_of(ff, 512), widths_of(d, 512), widths_of(d, d // 2)
        n, w, blocks = len(dw), dw[0][1], batch // BLOCK
        dma = pltpu.SemaphoreType.DMA
        scratch = [
            pltpu.VMEM((SLOTS, rows, head), BF16),
            pltpu.VMEM((SLOTS, rows, head), BF16),
            pltpu.VMEM((batch, d), BF16),
            pltpu.VMEM((d // 128, 128), BF16),
            pltpu.VMEM((d // 128, 128), BF16),
            pltpu.VMEM((2, 8, head), F32),
            pltpu.VMEM((batch, d), BF16),
            pltpu.VMEM((batch * heads, head), F32),
            pltpu.VMEM((GROUP, heads, rows), F32),
            pltpu.VMEM((GROUP, heads, rows), F32),
            pltpu.VMEM((batch * heads, head), F32),
            pltpu.VMEM((batch, d), F32),
            pltpu.VMEM((batch, d), F32),
            pltpu.VMEM((batch, ff), BF16),
            *[pltpu.VMEM((qcols, w), BF16) for _, w in ow],
            *[pltpu.VMEM((d, w), BF16) for _, w in ffw],
            *[pltpu.VMEM((d, w), BF16) for _, w in ffw],
            *[pltpu.VMEM((ff, w), BF16) for _, w in dw],
            pltpu.VMEM((2, blocks, BLOCK, d // 2), BF16),
            pltpu.VMEM((3, 2, blocks, BLOCK, d // 2), BF16),
            *[pltpu.VMEM((n, half, w), BF16) for _ in range(4)],
            dma((4,)),
            dma((2,)),
            dma((SLOTS,)),
            dma((SLOTS,)),
            dma((2,)),
            dma((len(ffw),)),
            dma((len(ffw),)),
            dma((n,)),
            dma((3, 2, blocks)),
            dma((3, 2, blocks)),
            *[dma((n,)) for _ in range(6)],
        ]
        hbm = pl.BlockSpec(memory_space=pltpu.HBM)
        return pl.pallas_call(
            functools.partial(layer, dims),
            out_shape=pltpu.VMEM((batch, d), BF16),
            in_specs=[hbm] * 11,
            out_specs=pl.BlockSpec(memory_space=pltpu.VMEM),
            scratch_shapes=scratch,
            compiler_params=pltpu.CompilerParams(collective_id=0, has_side_effects=True, vmem_limit_bytes=66000000),
            name="decoder_layer",
        )(
            x,
            k_cache.reshape(batch, rows, head),
            v_cache.reshape(batch, rows, head),
            gain_a.reshape(d // 128, 128),
            wq,
            wo,
            gain_m.reshape(d // 128, 128),
            w_gate,
            w_up,
            w_down,
            rotary(head, cache - 1),
        )

    states, cache, columns, rows_of = P("dp", None), P("dp", None, "tp", None), P(None, "tp"), P("tp", None)
    return jax.shard_map(
        step,
        mesh=mesh,
        in_specs=(states, cache, cache, P(None), columns, rows_of, P(None), columns, columns, rows_of),
        out_specs=states,
        check_vma=False,
    )
```

```python
import functools
import math

import jax
import jax.numpy as jnp
import numpy as np
from jax import lax
from jax.experimental import pallas as pl
from jax.experimental.pallas import tpu as pltpu
from jax.sharding import PartitionSpec as P

THETA = 10000
MESH = pl.DeviceIdType.MESH
F32, BF16 = jnp.float32, jnp.bfloat16

GROUP = 2
SLOTS = 8
LAG = 2
FIRST = 4
BLOCK = 8


def widths_of(total, width):
    return [(at, min(width, total - at)) for at in range(0, total, width)]


def rotary(head, place):
    half = head // 2
    angle = place * float(THETA) ** (-np.arange(half, dtype=np.float64) / half)
    cos, sin = np.cos(angle), np.sin(angle)
    rows = np.stack([np.concatenate([cos, cos]), np.concatenate([-sin, sin])])
    return np.broadcast_to(rows[:, None], (2, 8, head)).astype(np.float32)


def row_of(gain):
    wide = gain[...].astype(F32)
    return jnp.concatenate([wide[n : n + 1] for n in range(wide.shape[0])], -1)


def normed(x, gain):
    scale = lax.rsqrt(jnp.mean(x * x, -1, keepdims=True) + 1e-6)
    return (x * scale * gain).astype(BF16)


def layer(dims, x_hbm, k_hbm, v_hbm, ga_hbm, wq_hbm, wo_hbm, gm_hbm, wg_hbm, wu_hbm, wd_hbm, rot_hbm, y_ref, *scratch):
    batch, d, heads, kv, head, rows, ff = dims
    qcols = heads * head
    half = batch // 2
    ffw, dw, qw, ow = widths_of(ff, 512), widths_of(d, 512), widths_of(qcols, 512), widths_of(d, d // 2)
    it = iter(scratch)

    def take(n):
        return [next(it) for _ in range(n)]

    (kbuf, vbuf, xbuf, gab, gmb, rot, bbuf, qbuf, sa, sb, seen, states, wide, hidden) = take(14)
    wob = take(len(ow))
    gb, ub = take(len(ffw)), take(len(ffw))
    db = take(len(dw))
    terms, others, sends1, recvs1, sends2, recvs2 = take(6)
    (small_sem, wq_sem, k_sem, v_sem, wo_sem, g_sem, u_sem, d_sem, ts, tr, ss1, rs1, ss2, rs2, ss3, rs3) = take(16)

    tp = lax.axis_index("tp")
    core = lax.rem(tp, 2)
    chip = lax.div(tp, 2)
    partner = chip * 2 + 1 - core
    across = (1 - chip) * 2 + core
    diagonal = (1 - chip) * 2 + 1 - core
    peers = (partner, across, diagonal)

    barrier = pltpu.get_barrier_semaphore()
    for other in peers:
        pl.semaphore_signal(barrier, inc=1, device_id={"tp": other}, device_id_type=MESH)

    copy = pltpu.make_async_copy
    smalls = [copy(x_hbm, xbuf, small_sem.at[0]), copy(ga_hbm, gab, small_sem.at[1]), copy(gm_hbm, gmb, small_sem.at[2]), copy(rot_hbm, rot, small_sem.at[3])]
    for c in smalls:
        c.start()
    wqs = [copy(wq_hbm.at[:, pl.ds(at, w)], gb[i].at[:, pl.ds(0, w)], wq_sem.at[i]) for i, (at, w) in enumerate(qw)]
    for c in wqs:
        c.start()

    def k_copy(seq, slot):
        return copy(k_hbm.at[seq], kbuf.at[slot], k_sem.at[slot])

    def v_copy(seq, slot):
        return copy(v_hbm.at[seq], vbuf.at[slot], v_sem.at[slot])

    for s in range(FIRST):
        k_copy(s, s).start()
        v_copy(s, s).start()

    wos = [copy(wo_hbm.at[:, pl.ds(at, w)], wob[i], wo_sem.at[i]) for i, (at, w) in enumerate(ow)]
    gs = [copy(wg_hbm.at[:, pl.ds(at, w)], gb[i], g_sem.at[i]) for i, (at, w) in enumerate(ffw)]
    us = [copy(wu_hbm.at[:, pl.ds(at, w)], ub[i], u_sem.at[i]) for i, (at, w) in enumerate(ffw)]
    ds = [copy(wd_hbm.at[:, pl.ds(at, w)], db[i], d_sem.at[i]) for i, (at, w) in enumerate(dw)]

    for c in smalls:
        c.wait()
    states[...] = xbuf[...].astype(F32)
    bbuf[...] = normed(states[...], row_of(gab)).astype(BF16)
    cos, sin = rot[0, 0:1, :], rot[1, 0:1, :]
    for i, (at, w) in enumerate(qw):
        wqs[i].wait()
        if i == 0:
            for s in range(FIRST, SLOTS):
                k_copy(s, s).start()
                v_copy(s, s).start()
        q = jnp.dot(bbuf[...], gb[i][:, 0:w], preferred_element_type=F32)
        for n in range(w // head):
            t = q[:, n * head : (n + 1) * head].astype(BF16).astype(F32)
            t = t * cos + pltpu.roll(t, head // 2, 1) * sin
            qbuf[pl.ds(at // head + n, batch, stride=heads), :] = t.astype(BF16).astype(F32)

    groups = batch // GROUP
    ring = SLOTS // GROUP
    shape = (heads, rows)
    own = lax.rem(lax.broadcasted_iota(jnp.int32, shape, 1), kv) == lax.div(lax.broadcasted_iota(jnp.int32, shape, 0), heads // kv)
    factor = math.log2(math.e) * head**-0.5

    def slot_of(g, i):
        return lax.rem(g, ring) * GROUP + i

    def rows_of(g, i):
        return pl.ds(pl.multiple_of((g * GROUP + i) * heads, heads), heads)

    def scores_of(g, out):
        for i in range(GROUP):
            q = qbuf[rows_of(g, i), :].astype(BF16)
            out[i] = lax.dot_general(q, kbuf[slot_of(g, i)], (((1,), (1,)), ((), ())), preferred_element_type=F32)

    def weights_of(scores, i):
        s = jnp.where(own, scores[i], -jnp.inf)
        p = jnp.exp2((s - jnp.max(s, -1, keepdims=True)) * factor)
        return (p * (1.0 / jnp.sum(p, -1, keepdims=True))).astype(BF16)

    def seen_of(g, i, p):
        o = jnp.dot(p, vbuf[slot_of(g, i)], preferred_element_type=F32)
        seen[rows_of(g, i), :] = o.astype(BF16).astype(F32)

    def wait_k(g):
        for i in range(GROUP):
            k_copy(g * GROUP + i, slot_of(g, i)).wait()

    def wait_v(g, i):
        v_copy(g * GROUP + i, slot_of(g, i)).wait()

    def start_k(g):
        for i in range(GROUP):
            k_copy(g * GROUP + i, slot_of(g, i)).start()

    def start_v(g):
        for i in range(GROUP):
            v_copy(g * GROUP + i, slot_of(g, i)).start()

    def step(g, now, later):
        wait_k(g + 1)
        for i in range(GROUP):
            wait_v(g, i)
        scores_of(g + 1, later)
        for i in range(GROUP):
            seen_of(g, i, weights_of(now, i))

        @pl.when(g + 1 + ring < groups)
        def _():
            start_k(g + 1 + ring)

        @pl.when(g + ring < groups)
        def _():
            start_v(g + ring)

        @pl.when(g + ring == groups)
        def _():
            for c in [c for pair in zip(gs, us) for c in pair]:
                c.start(priority=1)

    def tail(g, now, later):
        wait_k(g + 1)
        scores_of(g + 1, later)
        ps = [weights_of(scores, i) for scores in (now, later) for i in range(GROUP)]
        for m in range(2):
            for i in range(GROUP):
                wait_v(g + m, i)
                seen_of(g + m, i, ps[m * GROUP + i])

    def remote(src, dst, send, recv, to):
        return pltpu.make_async_remote_copy(src_ref=src, dst_ref=dst, send_sem=send, recv_sem=recv, device_id={"tp": to}, device_id_type=MESH)

    def exchanges(b, n, c):
        at = pl.ds(b, n)
        return [remote(terms.at[c, at], others.at[p, c, at], ts.at[p, c, b], tr.at[p, c, b], to) for p, to in enumerate(peers)]

    def send_terms(b, n):
        rows = n * BLOCK
        block = [seen[pl.ds(b * (BLOCK * heads) + m, rows, stride=heads), :] for m in range(heads)]
        block = jnp.concatenate(block, -1).astype(BF16)
        for c, (at, w) in enumerate(ow):
            term = jnp.dot(block, wob[c][...], preferred_element_type=F32)
            terms[c, pl.ds(b, n)] = term.reshape(n, BLOCK, w).astype(BF16)
            for e in exchanges(b, n, c):
                e.start()

    def add_terms(b, n):
        rows = n * BLOCK
        at_rows = pl.ds(b * BLOCK, rows)
        squares = jnp.zeros((rows, 1), F32)
        for c, (at, w) in enumerate(ow):
            for e in exchanges(b, n, c):
                e.wait()
            t = [terms[c, pl.ds(b, n)]] + [others[p, c, pl.ds(b, n)] for p in range(3)]
            t = [v.astype(F32).reshape(rows, w) for v in t]
            h = states[at_rows, at : at + w] + ((t[0] + t[1]) + (t[2] + t[3]))
            h = h.astype(BF16).astype(F32)
            states[at_rows, at : at + w] = h
            squares = squares + jnp.sum(h * h, -1, keepdims=True)
        scale = lax.rsqrt(squares * (1.0 / d) + 1e-6)
        wide[at_rows, :] = states[at_rows, :] * scale * row_of(gmb)

    wait_k(0)
    scores_of(0, sa)
    start_k(ring)
    for c in wos:
        c.start()
    pl.semaphore_wait(barrier, 3)
    trips, blocks = groups // 2, batch // BLOCK
    ahead = 2 * BLOCK // (2 * GROUP)
    early = blocks - 2

    def two(i, carry):
        step(2 * i, sa, sb)
        step(2 * i + 1, sb, sa)

        @pl.when(i == ahead - 1)
        def _():
            for c in wos:
                c.wait()

        @pl.when(jnp.logical_and(lax.rem(i, ahead) == ahead - 1, i < trips - ahead))
        def _():
            send_terms(lax.div(i, ahead) * 2, 2)

        @pl.when(i == trips - 1 - ahead // 2)
        def _():
            send_terms(early, 1)

        return carry

    lax.fori_loop(0, trips - 1, two, 0)
    tail(groups - 2, sa, sb)
    send_terms(blocks - 1, 1)
    for c in ds:
        c.start(priority=1)
    for b in range(0, early, 2):
        add_terms(b, 2)
    add_terms(early, 1)
    add_terms(early + 1, 1)
    bbuf[...] = wide[...].astype(BF16)

    for c, (at, w) in enumerate(ffw):
        gs[c].wait()
        us[c].wait()
        gate = jnp.dot(bbuf[...], gb[c][...], preferred_element_type=F32)
        up = jnp.dot(bbuf[...], ub[c][...], preferred_element_type=F32)
        hidden[:, at : at + w] = (gate * (1.0 / (1.0 + jnp.exp(-gate))) * up).astype(BF16)

    which = lax.rem(core + chip, 2)
    mine = pl.ds(pl.multiple_of(which * half, half), half)
    theirs = pl.ds(pl.multiple_of((1 - which) * half, half), half)
    n = len(dw)
    one = [remote(sends1.at[c], recvs1.at[c], ss1.at[c], rs1.at[c], partner) for c in range(n)]
    two = [remote(sends2.at[c], recvs2.at[c], ss2.at[c], rs2.at[c], diagonal) for c in range(n)]
    spots = [y_ref.at[mine, pl.ds(at, w)] for at, w in dw]
    three = [remote(spots[c], spots[c], ss3.at[c], rs3.at[c], partner) for c in range(n)]

    def send_half(c):
        at, w = dw[c]
        wide[:, at : at + w] = jnp.dot(hidden[...], db[c][...], preferred_element_type=F32)
        sends1[c] = wide[theirs, at : at + w].astype(BF16)
        one[c].start()

    def send_chip(c):
        at, w = dw[c]
        one[c].wait_recv()
        sends2[c] = (wide[mine, at : at + w] + recvs1[c].astype(F32)).astype(BF16)
        two[c].start()

    def finish(c):
        at, w = dw[c]
        two[c].wait_recv()
        y_ref[mine, at : at + w] = (states[mine, at : at + w] + (sends2[c].astype(F32) + recvs2[c].astype(F32))).astype(BF16)
        three[c].start()

    for c in range(n + LAG):
        if c < n:
            ds[c].wait()
            send_half(c)
        if c >= LAG:
            send_chip(c - LAG)
    for c in range(n):
        finish(c)
    for c in range(n):
        three[c].wait()
        one[c].wait_send()
        two[c].wait_send()


def solution(mesh):
    def step(x, k_cache, v_cache, gain_a, wq, wo, gain_m, w_gate, w_up, w_down):
        batch, cache, kv, head = k_cache.shape
        d, qcols = wq.shape
        heads, ff, rows = qcols // head, w_gate.shape[1], cache * kv
        dims = (batch, d, heads, kv, head, rows, ff)
        half = batch // 2
        ffw, dw, ow = widths_of(ff, 512), widths_of(d, 512), widths_of(d, d // 2)
        n, w, blocks = len(dw), dw[0][1], batch // BLOCK
        dma = pltpu.SemaphoreType.DMA
        scratch = [
            pltpu.VMEM((SLOTS, rows, head), BF16),
            pltpu.VMEM((SLOTS, rows, head), BF16),
            pltpu.VMEM((batch, d), BF16),
            pltpu.VMEM((d // 128, 128), BF16),
            pltpu.VMEM((d // 128, 128), BF16),
            pltpu.VMEM((2, 8, head), F32),
            pltpu.VMEM((batch, d), BF16),
            pltpu.VMEM((batch * heads, head), F32),
            pltpu.VMEM((GROUP, heads, rows), F32),
            pltpu.VMEM((GROUP, heads, rows), F32),
            pltpu.VMEM((batch * heads, head), F32),
            pltpu.VMEM((batch, d), F32),
            pltpu.VMEM((batch, d), F32),
            pltpu.VMEM((batch, ff), BF16),
            *[pltpu.VMEM((qcols, w), BF16) for _, w in ow],
            *[pltpu.VMEM((d, w), BF16) for _, w in ffw],
            *[pltpu.VMEM((d, w), BF16) for _, w in ffw],
            *[pltpu.VMEM((ff, w), BF16) for _, w in dw],
            pltpu.VMEM((2, blocks, BLOCK, d // 2), BF16),
            pltpu.VMEM((3, 2, blocks, BLOCK, d // 2), BF16),
            *[pltpu.VMEM((n, half, w), BF16) for _ in range(4)],
            dma((4,)),
            dma((2,)),
            dma((SLOTS,)),
            dma((SLOTS,)),
            dma((2,)),
            dma((len(ffw),)),
            dma((len(ffw),)),
            dma((n,)),
            dma((3, 2, blocks)),
            dma((3, 2, blocks)),
            *[dma((n,)) for _ in range(6)],
        ]
        hbm = pl.BlockSpec(memory_space=pltpu.HBM)
        return pl.pallas_call(
            functools.partial(layer, dims),
            out_shape=pltpu.VMEM((batch, d), BF16),
            in_specs=[hbm] * 11,
            out_specs=pl.BlockSpec(memory_space=pltpu.VMEM),
            scratch_shapes=scratch,
            compiler_params=pltpu.CompilerParams(collective_id=0, has_side_effects=True, vmem_limit_bytes=66000000),
            name="decoder_layer",
        )(
            x,
            k_cache.reshape(batch, rows, head),
            v_cache.reshape(batch, rows, head),
            gain_a.reshape(d // 128, 128),
            wq,
            wo,
            gain_m.reshape(d // 128, 128),
            w_gate,
            w_up,
            w_down,
            rotary(head, cache - 1),
        )

    states, cache, columns, rows_of = P("dp", None), P("dp", None, "tp", None), P(None, "tp"), P("tp", None)
    return jax.shard_map(
        step,
        mesh=mesh,
        in_specs=(states, cache, cache, P(None), columns, rows_of, P(None), columns, columns, rows_of),
        out_specs=states,
        check_vma=False,
    )
```

```python
import functools
import math

import jax
import jax.numpy as jnp
import numpy as np
from jax import lax
from jax.experimental import pallas as pl
from jax.experimental.pallas import tpu as pltpu
from jax.sharding import PartitionSpec as P

THETA = 10000
MESH = pl.DeviceIdType.MESH
F32, BF16 = jnp.float32, jnp.bfloat16

GROUP = 2
SLOTS = 8
LAG = 2
FIRST = 4
BLOCK = 8


def widths_of(total, width):
    return [(at, min(width, total - at)) for at in range(0, total, width)]


def rotary(head, place):
    half = head // 2
    angle = place * float(THETA) ** (-np.arange(half, dtype=np.float64) / half)
    cos, sin = np.cos(angle), np.sin(angle)
    rows = np.stack([np.concatenate([cos, cos]), np.concatenate([-sin, sin])])
    return np.broadcast_to(rows[:, None], (2, 8, head)).astype(np.float32)


def row_of(gain):
    wide = gain[...].astype(F32)
    return jnp.concatenate([wide[n : n + 1] for n in range(wide.shape[0])], -1)


def normed(x, gain):
    scale = lax.rsqrt(jnp.mean(x * x, -1, keepdims=True) + 1e-6)
    return (x * scale * gain).astype(BF16)


def layer(dims, x_hbm, k_hbm, v_hbm, ga_hbm, wq_hbm, wo_hbm, gm_hbm, wg_hbm, wu_hbm, wd_hbm, rot_hbm, y_ref, *scratch):
    batch, d, heads, kv, head, rows, ff = dims
    qcols = heads * head
    half = batch // 2
    ffw, dw, qw, ow = widths_of(ff, 1024), widths_of(d, 512), widths_of(qcols, 512), widths_of(d, d)
    it = iter(scratch)

    def take(n):
        return [next(it) for _ in range(n)]

    (kbuf, vbuf, xbuf, gab, gmb, rot, bbuf, qbuf, sa, sb, seen, states, wide, hidden) = take(14)
    wob = take(len(ow))
    gb, ub = take(len(ffw)), take(len(ffw))
    db = take(len(dw))
    terms, others, sends1, recvs1, sends2, recvs2 = take(6)
    (small_sem, wq_sem, k_sem, v_sem, wo_sem, g_sem, u_sem, d_sem, ts, tr, ss1, rs1, ss2, rs2, ss3, rs3) = take(16)

    tp = lax.axis_index("tp")
    core = lax.rem(tp, 2)
    chip = lax.div(tp, 2)
    partner = chip * 2 + 1 - core
    across = (1 - chip) * 2 + core
    diagonal = (1 - chip) * 2 + 1 - core
    peers = (partner, across, diagonal)

    barrier = pltpu.get_barrier_semaphore()
    for other in peers:
        pl.semaphore_signal(barrier, inc=1, device_id={"tp": other}, device_id_type=MESH)

    copy = pltpu.make_async_copy
    smalls = [copy(x_hbm, xbuf, small_sem.at[0]), copy(ga_hbm, gab, small_sem.at[1]), copy(gm_hbm, gmb, small_sem.at[2]), copy(rot_hbm, rot, small_sem.at[3])]
    for c in smalls:
        c.start()
    wqs = [copy(wq_hbm.at[:, pl.ds(at, w)], gb[i].at[:, pl.ds(0, w)], wq_sem.at[i]) for i, (at, w) in enumerate(qw)]
    for c in wqs:
        c.start()

    def k_copy(seq, slot):
        return copy(k_hbm.at[seq], kbuf.at[slot], k_sem.at[slot])

    def v_copy(seq, slot):
        return copy(v_hbm.at[seq], vbuf.at[slot], v_sem.at[slot])

    for s in range(FIRST):
        k_copy(s, s).start()
        v_copy(s, s).start()

    wos = [copy(wo_hbm.at[:, pl.ds(at, w)], wob[i], wo_sem.at[i]) for i, (at, w) in enumerate(ow)]
    gs = [copy(wg_hbm.at[:, pl.ds(at, w)], gb[i], g_sem.at[i]) for i, (at, w) in enumerate(ffw)]
    us = [copy(wu_hbm.at[:, pl.ds(at, w)], ub[i], u_sem.at[i]) for i, (at, w) in enumerate(ffw)]
    ds = [copy(wd_hbm.at[:, pl.ds(at, w)], db[i], d_sem.at[i]) for i, (at, w) in enumerate(dw)]

    for c in smalls:
        c.wait()
    states[...] = xbuf[...].astype(F32)
    bbuf[...] = normed(states[...], row_of(gab)).astype(BF16)
    cos, sin = rot[0, 0:1, :], rot[1, 0:1, :]
    for i, (at, w) in enumerate(qw):
        wqs[i].wait()
        if i == 0:
            for s in range(FIRST, SLOTS):
                k_copy(s, s).start()
                v_copy(s, s).start()
        q = jnp.dot(bbuf[...], gb[i][:, 0:w], preferred_element_type=F32)
        for n in range(w // head):
            t = q[:, n * head : (n + 1) * head].astype(BF16).astype(F32)
            t = t * cos + pltpu.roll(t, head // 2, 1) * sin
            qbuf[pl.ds(at // head + n, batch, stride=heads), :] = t.astype(BF16).astype(F32)

    groups = batch // GROUP
    ring = SLOTS // GROUP
    shape = (heads, rows)
    own = lax.rem(lax.broadcasted_iota(jnp.int32, shape, 1), kv) == lax.div(lax.broadcasted_iota(jnp.int32, shape, 0), heads // kv)
    factor = math.log2(math.e) * head**-0.5

    def slot_of(g, i):
        return lax.rem(g, ring) * GROUP + i

    def rows_of(g, i):
        return pl.ds(pl.multiple_of((g * GROUP + i) * heads, heads), heads)

    def scores_of(g, out):
        for i in range(GROUP):
            q = qbuf[rows_of(g, i), :].astype(BF16)
            out[i] = lax.dot_general(q, kbuf[slot_of(g, i)], (((1,), (1,)), ((), ())), preferred_element_type=F32)

    def weights_of(scores, i):
        s = jnp.where(own, scores[i], -jnp.inf)
        p = jnp.exp2((s - jnp.max(s, -1, keepdims=True)) * factor)
        return (p * (1.0 / jnp.sum(p, -1, keepdims=True))).astype(BF16)

    def seen_of(g, i, p):
        o = jnp.dot(p, vbuf[slot_of(g, i)], preferred_element_type=F32)
        seen[rows_of(g, i), :] = o.astype(BF16).astype(F32)

    def wait_k(g):
        for i in range(GROUP):
            k_copy(g * GROUP + i, slot_of(g, i)).wait()

    def wait_v(g, i):
        v_copy(g * GROUP + i, slot_of(g, i)).wait()

    def start_k(g):
        for i in range(GROUP):
            k_copy(g * GROUP + i, slot_of(g, i)).start()

    def start_v(g):
        for i in range(GROUP):
            v_copy(g * GROUP + i, slot_of(g, i)).start()

    def step(g, now, later):
        wait_k(g + 1)
        for i in range(GROUP):
            wait_v(g, i)
        scores_of(g + 1, later)
        for i in range(GROUP):
            seen_of(g, i, weights_of(now, i))

        @pl.when(g + 1 + ring < groups)
        def _():
            start_k(g + 1 + ring)

        @pl.when(g + ring < groups)
        def _():
            start_v(g + ring)

        @pl.when(g + ring == groups)
        def _():
            for c in [c for pair in zip(gs, us) for c in pair]:
                c.start(priority=1)

    def tail(g, now, later):
        wait_k(g + 1)
        scores_of(g + 1, later)
        ps = [weights_of(scores, i) for scores in (now, later) for i in range(GROUP)]
        for m in range(2):
            for i in range(GROUP):
                wait_v(g + m, i)
                seen_of(g + m, i, ps[m * GROUP + i])

    def remote(src, dst, send, recv, to):
        return pltpu.make_async_remote_copy(src_ref=src, dst_ref=dst, send_sem=send, recv_sem=recv, device_id={"tp": to}, device_id_type=MESH)

    def exchanges(b, n, c):
        at = pl.ds(b, n)
        return [remote(terms.at[c, at], others.at[p, c, at], ts.at[p, c, b], tr.at[p, c, b], to) for p, to in enumerate(peers)]

    def send_terms(b, n):
        rows = n * BLOCK
        block = [seen[pl.ds(b * (BLOCK * heads) + m, rows, stride=heads), :] for m in range(heads)]
        block = jnp.concatenate(block, -1).astype(BF16)
        for c, (at, w) in enumerate(ow):
            term = jnp.dot(block, wob[c][...], preferred_element_type=F32)
            terms[c, pl.ds(b, n)] = term.reshape(n, BLOCK, w).astype(BF16)
            for e in exchanges(b, n, c):
                e.start()

    def add_terms(b, n):
        rows = n * BLOCK
        at_rows = pl.ds(b * BLOCK, rows)
        squares = jnp.zeros((rows, 1), F32)
        for c, (at, w) in enumerate(ow):
            for e in exchanges(b, n, c):
                e.wait()
            t = [terms[c, pl.ds(b, n)]] + [others[p, c, pl.ds(b, n)] for p in range(3)]
            t = [v.astype(F32).reshape(rows, w) for v in t]
            h = states[at_rows, at : at + w] + ((t[0] + t[1]) + (t[2] + t[3]))
            h = h.astype(BF16).astype(F32)
            states[at_rows, at : at + w] = h
            squares = squares + jnp.sum(h * h, -1, keepdims=True)
        scale = lax.rsqrt(squares * (1.0 / d) + 1e-6)
        wide[at_rows, :] = states[at_rows, :] * scale * row_of(gmb)

    wait_k(0)
    scores_of(0, sa)
    start_k(ring)
    for c in wos:
        c.start()
    pl.semaphore_wait(barrier, 3)
    trips, blocks = groups // 2, batch // BLOCK
    ahead = 2 * BLOCK // (2 * GROUP)
    early = blocks - 2

    def two(i, carry):
        step(2 * i, sa, sb)
        step(2 * i + 1, sb, sa)

        @pl.when(i == ahead - 1)
        def _():
            for c in wos:
                c.wait()

        @pl.when(jnp.logical_and(lax.rem(i, ahead) == ahead - 1, i < trips - ahead))
        def _():
            send_terms(lax.div(i, ahead) * 2, 2)

        @pl.when(i == trips - 1 - ahead // 2)
        def _():
            send_terms(early, 1)

        return carry

    lax.fori_loop(0, trips - 1, two, 0)
    tail(groups - 2, sa, sb)
    send_terms(blocks - 1, 1)
    for c in ds:
        c.start(priority=1)
    for b in range(0, early, 2):
        add_terms(b, 2)
    add_terms(early, 1)
    add_terms(early + 1, 1)
    bbuf[...] = wide[...].astype(BF16)

    for c, (at, w) in enumerate(ffw):
        gs[c].wait()
        us[c].wait()
        gate = jnp.dot(bbuf[...], gb[c][...], preferred_element_type=F32)
        up = jnp.dot(bbuf[...], ub[c][...], preferred_element_type=F32)
        hidden[:, at : at + w] = (gate * (1.0 / (1.0 + jnp.exp(-gate))) * up).astype(BF16)

    which = lax.rem(core + chip, 2)
    mine = pl.ds(pl.multiple_of(which * half, half), half)
    theirs = pl.ds(pl.multiple_of((1 - which) * half, half), half)
    n = len(dw)
    one = [remote(sends1.at[c], recvs1.at[c], ss1.at[c], rs1.at[c], partner) for c in range(n)]
    two = [remote(sends2.at[c], recvs2.at[c], ss2.at[c], rs2.at[c], diagonal) for c in range(n)]
    spots = [y_ref.at[mine, pl.ds(at, w)] for at, w in dw]
    three = [remote(spots[c], spots[c], ss3.at[c], rs3.at[c], partner) for c in range(n)]

    def send_half(c):
        at, w = dw[c]
        wide[:, at : at + w] = jnp.dot(hidden[...], db[c][...], preferred_element_type=F32)
        sends1[c] = wide[theirs, at : at + w].astype(BF16)
        one[c].start()

    def send_chip(c):
        at, w = dw[c]
        one[c].wait_recv()
        sends2[c] = (wide[mine, at : at + w] + recvs1[c].astype(F32)).astype(BF16)
        two[c].start()

    def finish(c):
        at, w = dw[c]
        two[c].wait_recv()
        y_ref[mine, at : at + w] = (states[mine, at : at + w] + (sends2[c].astype(F32) + recvs2[c].astype(F32))).astype(BF16)
        three[c].start()

    for c in range(n + LAG):
        if c < n:
            ds[c].wait()
            send_half(c)
        if c >= LAG:
            send_chip(c - LAG)
    for c in range(n):
        finish(c)
    for c in range(n):
        three[c].wait()
        one[c].wait_send()
        two[c].wait_send()


def solution(mesh):
    def step(x, k_cache, v_cache, gain_a, wq, wo, gain_m, w_gate, w_up, w_down):
        batch, cache, kv, head = k_cache.shape
        d, qcols = wq.shape
        heads, ff, rows = qcols // head, w_gate.shape[1], cache * kv
        dims = (batch, d, heads, kv, head, rows, ff)
        half = batch // 2
        ffw, dw, ow = widths_of(ff, 1024), widths_of(d, 512), widths_of(d, d)
        n, w, blocks = len(dw), dw[0][1], batch // BLOCK
        dma = pltpu.SemaphoreType.DMA
        scratch = [
            pltpu.VMEM((SLOTS, rows, head), BF16),
            pltpu.VMEM((SLOTS, rows, head), BF16),
            pltpu.VMEM((batch, d), BF16),
            pltpu.VMEM((d // 128, 128), BF16),
            pltpu.VMEM((d // 128, 128), BF16),
            pltpu.VMEM((2, 8, head), F32),
            pltpu.VMEM((batch, d), BF16),
            pltpu.VMEM((batch * heads, head), F32),
            pltpu.VMEM((GROUP, heads, rows), F32),
            pltpu.VMEM((GROUP, heads, rows), F32),
            pltpu.VMEM((batch * heads, head), F32),
            pltpu.VMEM((batch, d), F32),
            pltpu.VMEM((batch, d), F32),
            pltpu.VMEM((batch, ff), BF16),
            *[pltpu.VMEM((qcols, w), BF16) for _, w in ow],
            *[pltpu.VMEM((d, w), BF16) for _, w in ffw],
            *[pltpu.VMEM((d, w), BF16) for _, w in ffw],
            *[pltpu.VMEM((ff, w), BF16) for _, w in dw],
            pltpu.VMEM((1, blocks, BLOCK, d), BF16),
            pltpu.VMEM((3, 1, blocks, BLOCK, d), BF16),
            *[pltpu.VMEM((n, half, w), BF16) for _ in range(4)],
            dma((4,)),
            dma((2,)),
            dma((SLOTS,)),
            dma((SLOTS,)),
            dma((2,)),
            dma((len(ffw),)),
            dma((len(ffw),)),
            dma((n,)),
            dma((3, 1, blocks)),
            dma((3, 1, blocks)),
            *[dma((n,)) for _ in range(6)],
        ]
        hbm = pl.BlockSpec(memory_space=pltpu.HBM)
        return pl.pallas_call(
            functools.partial(layer, dims),
            out_shape=pltpu.VMEM((batch, d), BF16),
            in_specs=[hbm] * 11,
            out_specs=pl.BlockSpec(memory_space=pltpu.VMEM),
            scratch_shapes=scratch,
            compiler_params=pltpu.CompilerParams(collective_id=0, has_side_effects=True, vmem_limit_bytes=66000000),
            name="decoder_layer",
        )(
            x,
            k_cache.reshape(batch, rows, head),
            v_cache.reshape(batch, rows, head),
            gain_a.reshape(d // 128, 128),
            wq,
            wo,
            gain_m.reshape(d // 128, 128),
            w_gate,
            w_up,
            w_down,
            rotary(head, cache - 1),
        )

    states, cache, columns, rows_of = P("dp", None), P("dp", None, "tp", None), P(None, "tp"), P("tp", None)
    return jax.shard_map(
        step,
        mesh=mesh,
        in_specs=(states, cache, cache, P(None), columns, rows_of, P(None), columns, columns, rows_of),
        out_specs=states,
        check_vma=False,
    )
```

```python
import functools
import math

import jax
import jax.numpy as jnp
import numpy as np
from jax import lax
from jax.experimental import pallas as pl
from jax.experimental.pallas import tpu as pltpu
from jax.sharding import PartitionSpec as P

THETA = 10000
MESH = pl.DeviceIdType.MESH
F32, BF16 = jnp.float32, jnp.bfloat16

GROUP = 2
SLOTS = 8
LAG = 2
FIRST = 4
BLOCK = 8


def widths_of(total, width):
    return [(at, min(width, total - at)) for at in range(0, total, width)]


def rotary(head, place):
    half = head // 2
    angle = place * float(THETA) ** (-np.arange(half, dtype=np.float64) / half)
    cos, sin = np.cos(angle), np.sin(angle)
    rows = np.stack([np.concatenate([cos, cos]), np.concatenate([-sin, sin])])
    return np.broadcast_to(rows[:, None], (2, 8, head)).astype(np.float32)


def row_of(gain):
    wide = gain[...].astype(F32)
    return jnp.concatenate([wide[n : n + 1] for n in range(wide.shape[0])], -1)


def normed(x, gain):
    scale = lax.rsqrt(jnp.mean(x * x, -1, keepdims=True) + 1e-6)
    return (x * scale * gain).astype(BF16)


def layer(dims, x_hbm, k_hbm, v_hbm, ga_hbm, wq_hbm, wo_hbm, gm_hbm, wg_hbm, wu_hbm, wd_hbm, rot_hbm, y_ref, *scratch):
    batch, d, heads, kv, head, rows, ff = dims
    qcols = heads * head
    half = batch // 2
    ffw, dw, qw, ow = widths_of(ff, 1024), widths_of(d, 512), widths_of(qcols, 512), widths_of(d, d)
    it = iter(scratch)

    def take(n):
        return [next(it) for _ in range(n)]

    (kbuf, vbuf, xbuf, gab, gmb, rot, bbuf, qbuf, sa, sb, seen, states, wide, hidden) = take(14)
    wob = take(len(ow))
    gb, ub = take(len(ffw)), take(len(ffw))
    db = take(len(dw))
    terms, others, sends1, recvs1, sends2, recvs2 = take(6)
    (small_sem, wq_sem, k_sem, v_sem, wo_sem, g_sem, u_sem, d_sem, ts, tr, ss1, rs1, ss2, rs2, ss3, rs3) = take(16)

    tp = lax.axis_index("tp")
    core = lax.rem(tp, 2)
    chip = lax.div(tp, 2)
    partner = chip * 2 + 1 - core
    across = (1 - chip) * 2 + core
    diagonal = (1 - chip) * 2 + 1 - core
    peers = (partner, across, diagonal)

    barrier = pltpu.get_barrier_semaphore()
    for other in peers:
        pl.semaphore_signal(barrier, inc=1, device_id={"tp": other}, device_id_type=MESH)

    copy = pltpu.make_async_copy
    smalls = [copy(x_hbm, xbuf, small_sem.at[0]), copy(ga_hbm, gab, small_sem.at[1]), copy(gm_hbm, gmb, small_sem.at[2]), copy(rot_hbm, rot, small_sem.at[3])]
    for c in smalls:
        c.start()
    wqs = [copy(wq_hbm.at[:, pl.ds(at, w)], gb[i].at[:, pl.ds(0, w)], wq_sem.at[i]) for i, (at, w) in enumerate(qw)]
    for c in wqs:
        c.start()

    def k_copy(seq, slot):
        return copy(k_hbm.at[seq], kbuf.at[slot], k_sem.at[slot])

    def v_copy(seq, slot):
        return copy(v_hbm.at[seq], vbuf.at[slot], v_sem.at[slot])

    for s in range(FIRST):
        k_copy(s, s).start()
        v_copy(s, s).start()

    wos = [copy(wo_hbm.at[:, pl.ds(at, w)], wob[i], wo_sem.at[i]) for i, (at, w) in enumerate(ow)]
    gs = [copy(wg_hbm.at[:, pl.ds(at, w)], gb[i], g_sem.at[i]) for i, (at, w) in enumerate(ffw)]
    us = [copy(wu_hbm.at[:, pl.ds(at, w)], ub[i], u_sem.at[i]) for i, (at, w) in enumerate(ffw)]
    ds = [copy(wd_hbm.at[:, pl.ds(at, w)], db[i], d_sem.at[i]) for i, (at, w) in enumerate(dw)]

    for c in smalls:
        c.wait()
    states[...] = xbuf[...].astype(F32)
    bbuf[...] = normed(states[...], row_of(gab)).astype(BF16)
    cos, sin = rot[0, 0:1, :], rot[1, 0:1, :]
    for i, (at, w) in enumerate(qw):
        wqs[i].wait()
        if i == 0:
            for s in range(FIRST, SLOTS):
                k_copy(s, s).start()
                v_copy(s, s).start()
        q = jnp.dot(bbuf[...], gb[i][:, 0:w], preferred_element_type=F32)
        for n in range(w // head):
            t = q[:, n * head : (n + 1) * head].astype(BF16).astype(F32)
            t = t * cos + pltpu.roll(t, head // 2, 1) * sin
            qbuf[pl.ds(at // head + n, batch, stride=heads), :] = t.astype(BF16).astype(F32)

    groups = batch // GROUP
    ring = SLOTS // GROUP
    shape = (heads, rows)
    own = lax.rem(lax.broadcasted_iota(jnp.int32, shape, 1), kv) == lax.div(lax.broadcasted_iota(jnp.int32, shape, 0), heads // kv)
    factor = math.log2(math.e) * head**-0.5

    def slot_of(g, i):
        return lax.rem(g, ring) * GROUP + i

    def rows_of(g, i):
        return pl.ds(pl.multiple_of((g * GROUP + i) * heads, heads), heads)

    def scores_of(g, out):
        for i in range(GROUP):
            q = qbuf[rows_of(g, i), :].astype(BF16)
            out[i] = lax.dot_general(q, kbuf[slot_of(g, i)], (((1,), (1,)), ((), ())), preferred_element_type=F32)

    def weights_of(scores, i):
        s = jnp.where(own, scores[i], -jnp.inf)
        p = jnp.exp2((s - jnp.max(s, -1, keepdims=True)) * factor)
        return (p * (1.0 / jnp.sum(p, -1, keepdims=True))).astype(BF16)

    def seen_of(g, i, p):
        o = jnp.dot(p, vbuf[slot_of(g, i)], preferred_element_type=F32)
        seen[rows_of(g, i), :] = o.astype(BF16).astype(F32)

    def wait_k(g):
        for i in range(GROUP):
            k_copy(g * GROUP + i, slot_of(g, i)).wait()

    def wait_v(g, i):
        v_copy(g * GROUP + i, slot_of(g, i)).wait()

    def start_k(g):
        for i in range(GROUP):
            k_copy(g * GROUP + i, slot_of(g, i)).start()

    def start_v(g):
        for i in range(GROUP):
            v_copy(g * GROUP + i, slot_of(g, i)).start()

    def step(g, now, later):
        wait_k(g + 1)
        for i in range(GROUP):
            wait_v(g, i)
        scores_of(g + 1, later)
        for i in range(GROUP):
            seen_of(g, i, weights_of(now, i))

        @pl.when(g + 1 + ring < groups)
        def _():
            start_k(g + 1 + ring)

        @pl.when(g + ring < groups)
        def _():
            start_v(g + ring)

        @pl.when(g + ring == groups)
        def _():
            for c in [c for pair in zip(gs, us) for c in pair]:
                c.start(priority=1)

    def tail(g, now, later):
        wait_k(g + 1)
        scores_of(g + 1, later)
        ps = [weights_of(scores, i) for scores in (now, later) for i in range(GROUP)]
        for m in range(2):
            for i in range(GROUP):
                wait_v(g + m, i)
                seen_of(g + m, i, ps[m * GROUP + i])

    def remote(src, dst, send, recv, to):
        return pltpu.make_async_remote_copy(src_ref=src, dst_ref=dst, send_sem=send, recv_sem=recv, device_id={"tp": to}, device_id_type=MESH)

    def exchanges(b, n, c):
        at = pl.ds(b, n)
        return [remote(terms.at[c, at], others.at[p, c, at], ts.at[p, c, b], tr.at[p, c, b], to) for p, to in enumerate(peers)]

    def send_terms(b, n):
        rows = n * BLOCK
        block = [seen[pl.ds(b * (BLOCK * heads) + m, rows, stride=heads), :] for m in range(heads)]
        block = jnp.concatenate(block, -1).astype(BF16)
        for c, (at, w) in enumerate(ow):
            term = jnp.dot(block, wob[c][...], preferred_element_type=F32)
            terms[c, pl.ds(b, n)] = term.reshape(n, BLOCK, w).astype(BF16)
            for e in exchanges(b, n, c):
                e.start()

    def add_terms(b, n):
        rows = n * BLOCK
        at_rows = pl.ds(b * BLOCK, rows)
        squares = jnp.zeros((rows, 1), F32)
        for c, (at, w) in enumerate(ow):
            for e in exchanges(b, n, c):
                e.wait()
            t = [terms[c, pl.ds(b, n)]] + [others[p, c, pl.ds(b, n)] for p in range(3)]
            t = [v.astype(F32).reshape(rows, w) for v in t]
            h = states[at_rows, at : at + w] + ((t[0] + t[1]) + (t[2] + t[3]))
            h = h.astype(BF16).astype(F32)
            states[at_rows, at : at + w] = h
            squares = squares + jnp.sum(h * h, -1, keepdims=True)
        scale = lax.rsqrt(squares * (1.0 / d) + 1e-6)
        wide[at_rows, :] = states[at_rows, :] * scale * row_of(gmb)

    wait_k(0)
    scores_of(0, sa)
    start_k(ring)
    for c in wos:
        c.start()
    pl.semaphore_wait(barrier, 3)
    trips, blocks = groups // 2, batch // BLOCK
    each = BLOCK // (2 * GROUP)
    first = 3 if blocks % 2 == 0 else 2

    def two(i, carry):
        step(2 * i, sa, sb)
        step(2 * i + 1, sb, sa)

        @pl.when(i == first * each - 1)
        def _():
            for c in wos:
                c.wait()
            send_terms(0, first)

        @pl.when(jnp.logical_and(i >= first * each, lax.rem(i - first * each, 2 * each) == 2 * each - 1))
        def _():
            send_terms(lax.div(i + 1, each) - 2, 2)

        return carry

    lax.fori_loop(0, trips - 1, two, 0)
    tail(groups - 2, sa, sb)
    send_terms(blocks - 1, 1)
    for c in ds:
        c.start(priority=1)
    add_terms(0, first)
    for b in range(first, blocks - 1, 2):
        add_terms(b, 2)
    add_terms(blocks - 1, 1)
    bbuf[...] = wide[...].astype(BF16)

    for c, (at, w) in enumerate(ffw):
        gs[c].wait()
        us[c].wait()
        gate = jnp.dot(bbuf[...], gb[c][...], preferred_element_type=F32)
        up = jnp.dot(bbuf[...], ub[c][...], preferred_element_type=F32)
        hidden[:, at : at + w] = (gate * (1.0 / (1.0 + jnp.exp(-gate))) * up).astype(BF16)

    which = lax.rem(core + chip, 2)
    mine = pl.ds(pl.multiple_of(which * half, half), half)
    theirs = pl.ds(pl.multiple_of((1 - which) * half, half), half)
    n = len(dw)
    one = [remote(sends1.at[c], recvs1.at[c], ss1.at[c], rs1.at[c], partner) for c in range(n)]
    two = [remote(sends2.at[c], recvs2.at[c], ss2.at[c], rs2.at[c], diagonal) for c in range(n)]
    spots = [y_ref.at[mine, pl.ds(at, w)] for at, w in dw]
    three = [remote(spots[c], spots[c], ss3.at[c], rs3.at[c], partner) for c in range(n)]

    def send_half(c):
        at, w = dw[c]
        wide[:, at : at + w] = jnp.dot(hidden[...], db[c][...], preferred_element_type=F32)
        sends1[c] = wide[theirs, at : at + w].astype(BF16)
        one[c].start()

    def send_chip(c):
        at, w = dw[c]
        one[c].wait_recv()
        sends2[c] = (wide[mine, at : at + w] + recvs1[c].astype(F32)).astype(BF16)
        two[c].start()

    def finish(c):
        at, w = dw[c]
        two[c].wait_recv()
        y_ref[mine, at : at + w] = (states[mine, at : at + w] + (sends2[c].astype(F32) + recvs2[c].astype(F32))).astype(BF16)
        three[c].start()

    for c in range(n + LAG):
        if c < n:
            ds[c].wait()
            send_half(c)
        if c >= LAG:
            send_chip(c - LAG)
    for c in range(n):
        finish(c)
    for c in range(n):
        three[c].wait()
        one[c].wait_send()
        two[c].wait_send()


def solution(mesh):
    def step(x, k_cache, v_cache, gain_a, wq, wo, gain_m, w_gate, w_up, w_down):
        batch, cache, kv, head = k_cache.shape
        d, qcols = wq.shape
        heads, ff, rows = qcols // head, w_gate.shape[1], cache * kv
        dims = (batch, d, heads, kv, head, rows, ff)
        half = batch // 2
        ffw, dw, ow = widths_of(ff, 1024), widths_of(d, 512), widths_of(d, d)
        n, w, blocks = len(dw), dw[0][1], batch // BLOCK
        dma = pltpu.SemaphoreType.DMA
        scratch = [
            pltpu.VMEM((SLOTS, rows, head), BF16),
            pltpu.VMEM((SLOTS, rows, head), BF16),
            pltpu.VMEM((batch, d), BF16),
            pltpu.VMEM((d // 128, 128), BF16),
            pltpu.VMEM((d // 128, 128), BF16),
            pltpu.VMEM((2, 8, head), F32),
            pltpu.VMEM((batch, d), BF16),
            pltpu.VMEM((batch * heads, head), F32),
            pltpu.VMEM((GROUP, heads, rows), F32),
            pltpu.VMEM((GROUP, heads, rows), F32),
            pltpu.VMEM((batch * heads, head), F32),
            pltpu.VMEM((batch, d), F32),
            pltpu.VMEM((batch, d), F32),
            pltpu.VMEM((batch, ff), BF16),
            *[pltpu.VMEM((qcols, w), BF16) for _, w in ow],
            *[pltpu.VMEM((d, w), BF16) for _, w in ffw],
            *[pltpu.VMEM((d, w), BF16) for _, w in ffw],
            *[pltpu.VMEM((ff, w), BF16) for _, w in dw],
            pltpu.VMEM((1, blocks, BLOCK, d), BF16),
            pltpu.VMEM((3, 1, blocks, BLOCK, d), BF16),
            *[pltpu.VMEM((n, half, w), BF16) for _ in range(4)],
            dma((4,)),
            dma((2,)),
            dma((SLOTS,)),
            dma((SLOTS,)),
            dma((2,)),
            dma((len(ffw),)),
            dma((len(ffw),)),
            dma((n,)),
            dma((3, 1, blocks)),
            dma((3, 1, blocks)),
            *[dma((n,)) for _ in range(6)],
        ]
        hbm = pl.BlockSpec(memory_space=pltpu.HBM)
        return pl.pallas_call(
            functools.partial(layer, dims),
            out_shape=pltpu.VMEM((batch, d), BF16),
            in_specs=[hbm] * 11,
            out_specs=pl.BlockSpec(memory_space=pltpu.VMEM),
            scratch_shapes=scratch,
            compiler_params=pltpu.CompilerParams(collective_id=0, has_side_effects=True, vmem_limit_bytes=66000000),
            name="decoder_layer",
        )(
            x,
            k_cache.reshape(batch, rows, head),
            v_cache.reshape(batch, rows, head),
            gain_a.reshape(d // 128, 128),
            wq,
            wo,
            gain_m.reshape(d // 128, 128),
            w_gate,
            w_up,
            w_down,
            rotary(head, cache - 1),
        )

    states, cache, columns, rows_of = P("dp", None), P("dp", None, "tp", None), P(None, "tp"), P("tp", None)
    return jax.shard_map(
        step,
        mesh=mesh,
        in_specs=(states, cache, cache, P(None), columns, rows_of, P(None), columns, columns, rows_of),
        out_specs=states,
        check_vma=False,
    )
```
